256 devices in a mesh: gx: 8 (over z), gy: 4 (over y), gz: 8 (over x, core).
Axes of the slice: x: 4, y: 4, z: 8, core: 2. Of those that a mesh axis runs over, the one named last changes fastest.
Arguments:
- schur: bfloat16 [8, 4, 8, 2048, 2048], P('gx', 'gy', 'gz'), may hold values from -0.09375 to 0.09375
- interface_diag: float32 [8, 4, 8, 2048], P('gx', 'gy', 'gz'), may hold values from 2 to 4
- precond: float32 [8, 4, 8, 16, 128, 128], P('gx', 'gy', 'gz'), may hold values from -0.3 to 0.8
- load: bfloat16 [8, 4, 8, 2048, 256], P('gx', 'gy', 'gz'), may hold values from -170 to 170
- face_blocks: int32 [8, 4, 8, 6, 2], P('gx', 'gy', 'gz'), may hold values from 0 to 16, as said below
Outputs:
- solution: float32 [8, 4, 8, 2048, 256], P('gx', 'gy', 'gz')
- residual_norm: float32 [256], replicated
The draws below stay inside these ranges and needn't reach their ends.
Inputs may be any that keep to these rules, and one draw needn't show every extreme that they name: `face_blocks`: for each subdomain p and direction d (0, 1: next and previous along the first grid dimension; 2, 3 and 4, 5 likewise along the second and third), slots 0 to n - 1 hold block numbers below 16 shared with the neighbour in that direction, where n (1 to 2 inside the grid, 0 across its boundary) equals the neighbour's n for the opposite direction, and the neighbour's slot k of the opposite direction holds the block that shares with p's slot k; the remaining slots hold 16; no block number appears twice in one subdomain's table; some face shares 2 blocks in every draw.
All inputs are finite; a program needn't handle non-finite values.
Results may differ from the reference program's by a relative error of at most 0.0008.
Values sent between devices are 32-bit elements; how exact they have to be, the bound alone decides.
A program may use at most 128 MiB of HBM per device.

```python
import math
import jax
import jax.numpy as jnp
from jax import lax

BLK = 128
NBLK = 16
IFACE = 2048
CAP = 2
NRHS = 256
SUB_X = 8
SUB_Y = 4
SUB_Z = 8


def draw_precond(key, part):
    full_shape = (SUB_X, SUB_Y, SUB_Z, NBLK, BLK, BLK)
    key_diag, key_off = jax.random.split(jax.random.fold_in(key, 11))
    diagonal = 1.0 / jax.random.uniform(key_diag, full_shape[:-1], jnp.float32, 2.0, 4.0)
    coupling = jnp.clip(jax.random.normal(key_off, full_shape, jnp.float32), -6.0, 6.0) * (0.12 / math.sqrt(BLK))
    identity = jnp.eye(BLK, dtype=jnp.float32)
    return coupling + diagonal[..., None] * identity


def ramp_factor(length):
    return jnp.power(3.0, jnp.arange(length, dtype=jnp.float32) / max(length - 1, 1))


def draw_load(key, part):
    key_base = jax.random.fold_in(jax.random.fold_in(key, 5), 0)
    key_rows = jax.random.fold_in(jax.random.fold_in(key, 5), 2)
    key_cols = jax.random.fold_in(jax.random.fold_in(key, 5), 3)
    full_shape = (SUB_X, SUB_Y, SUB_Z, NBLK * BLK, NRHS)
    row_scale = jnp.exp(jax.random.uniform(key_rows, full_shape[:4] + (1,), jnp.float32, 0.0, math.log(10.0)))
    col_scale = jnp.exp(jax.random.uniform(key_cols, (NRHS,), jnp.float32, 0.0, math.log(10.0)))
    position = ramp_factor(SUB_X)[:, None, None] * ramp_factor(SUB_Y)[None, :, None] * ramp_factor(SUB_Z)[None, None, :]
    base = jnp.clip(jax.random.normal(key_base, full_shape, jnp.float32), -6.0, 6.0)
    values = 0.01 * base * row_scale * col_scale * position[..., None, None]
    return values.astype(jnp.bfloat16)


def pair_counts(pair_key, axis_id):
    grid_shape = [SUB_X, SUB_Y, SUB_Z]
    grid_shape[axis_id] = grid_shape[axis_id] - 1
    counts = jax.random.randint(pair_key, tuple(grid_shape), 1, CAP + 1, dtype=jnp.int32)
    if grid_shape[axis_id] > 0:
        counts = counts.at[0, 0, 0].set(CAP)
    pad_upper = [(0, 0)] * 3
    pad_upper[axis_id] = (0, 1)
    pad_lower = [(0, 0)] * 3
    pad_lower[axis_id] = (1, 0)
    return (jnp.pad(counts, pad_upper), jnp.pad(counts, pad_lower))


def draw_face_blocks(key, part):
    key_x, key_y, key_z, key_perm = jax.random.split(jax.random.fold_in(key, 7), 4)
    upper_x, lower_x = pair_counts(key_x, 0)
    upper_y, lower_y = pair_counts(key_y, 1)
    upper_z, lower_z = pair_counts(key_z, 2)
    dir_counts = jnp.stack([upper_x, lower_x, upper_y, lower_y, upper_z, lower_z], axis=-1)
    offsets = jnp.cumsum(dir_counts, axis=-1) - dir_counts
    subdomains = SUB_X * SUB_Y * SUB_Z
    perm_keys = jax.random.split(key_perm, subdomains)
    orders = jax.vmap(lambda one_key: jax.random.permutation(one_key, NBLK))(perm_keys).astype(jnp.int32)
    orders = orders.reshape(SUB_X, SUB_Y, SUB_Z, 1, NBLK)
    slot_ids = jnp.arange(CAP, dtype=jnp.int32)
    positions = jnp.minimum(offsets[..., None] + slot_ids, NBLK - 1).astype(jnp.int32)
    picked = jnp.take_along_axis(orders, positions.reshape(SUB_X, SUB_Y, SUB_Z, 1, 6 * CAP), axis=-1)
    picked = picked.reshape(SUB_X, SUB_Y, SUB_Z, 6, CAP)
    valid = slot_ids < dir_counts[..., None]
    return jnp.where(valid, picked, NBLK).astype(jnp.int32)


def block_levels(own_key, shape, pieces, least, top_value):
    gain = 1.0
    for dim, parts in pieces:
        draws = jax.random.uniform(jax.random.fold_in(jax.random.fold_in(own_key, 6), dim), (parts,), jnp.float32, least / len(pieces), top_value / len(pieces))
        gain = gain * jnp.repeat(jnp.exp(draws), shape[dim] // parts).reshape((-1,) + (1,) * (len(shape) - 1 - dim))
    return gain


def gaussian(stream_key, shape, width, reach, shards=(), kind=jnp.bfloat16):
    result = width * jax.random.normal(stream_key, shape, jnp.float32)
    if shards:
        result = result * block_levels(stream_key, shape, shards, -0.22, 0.18)
    return jnp.clip(result, -reach, reach).astype(kind)


def setup_inputs(seed: int = 0) -> dict:
    seeds = jax.random.split(jax.random.key(seed), 6)
    return {
        "schur": gaussian(seeds[0], (SUB_X, SUB_Y, SUB_Z, IFACE, IFACE), (2 * IFACE) ** -0.5, 0.09375, ((0, 8), (1, 4), (2, 8))),
        "interface_diag": jnp.clip(jnp.exp(math.log(4.0) - 0.6931472 * jax.random.uniform(seeds[1], (SUB_X, SUB_Y, SUB_Z, IFACE), jnp.float32) ** block_levels(seeds[1], (SUB_X, SUB_Y, SUB_Z, IFACE), ((0, 8), (1, 4), (2, 8)), -0.2, 0.2)), 2.0, 4.0),
        "precond": draw_precond(jax.random.fold_in(seeds[5], 71), 0),
        "load": draw_load(jax.random.fold_in(seeds[5], 71), 0),
        "face_blocks": draw_face_blocks(jax.random.fold_in(seeds[5], 71), 0),
    }


epsilon = 1e-06

def find_live(face_blocks):
    slot_hits = face_blocks[..., None] == jnp.arange(NBLK, dtype=jnp.int32)
    return jnp.any(slot_hits, axis=(3, 4)).astype(jnp.float32)

def from_next(values, axis_id):
    length = values.shape[axis_id]
    pad_spec = [(0, 0)] * values.ndim
    pad_spec[axis_id] = (0, 1)
    return lax.slice_in_dim(jnp.pad(values, pad_spec), 1, length + 1, axis=axis_id)

def from_prev(values, axis_id):
    length = values.shape[axis_id]
    pad_spec = [(0, 0)] * values.ndim
    pad_spec[axis_id] = (1, 0)
    return lax.slice_in_dim(jnp.pad(values, pad_spec), 0, length, axis=axis_id)

def assemble(blocks, face_blocks, live_mask):
    grid_shape = blocks.shape[:3]
    row_width = blocks.shape[-1]
    subdomains = grid_shape[0] * grid_shape[1] * grid_shape[2]
    flattened = blocks.reshape(subdomains, NBLK, BLK, row_width)
    extended = jnp.concatenate([flattened, jnp.zeros((subdomains, 1, BLK, row_width), jnp.float32)], axis=1)
    slot_index = face_blocks.reshape(subdomains, 6 * CAP).astype(jnp.int32)
    packed = jax.vmap(lambda table, picks: table[picks])(extended, slot_index)
    packed = packed.reshape(grid_shape + (6, CAP, BLK, row_width))
    arrived = jnp.stack([from_next(packed[:, :, :, 1], 0), from_prev(packed[:, :, :, 0], 0), from_next(packed[:, :, :, 3], 1), from_prev(packed[:, :, :, 2], 1), from_next(packed[:, :, :, 5], 2), from_prev(packed[:, :, :, 4], 2)], axis=3)
    arrived = arrived.reshape(subdomains, 6 * CAP, BLK, row_width)
    extended = jax.vmap(lambda table, picks, extra: table.at[picks].add(extra))(extended, slot_index, arrived)
    return extended[:, :NBLK].reshape(blocks.shape) * live_mask[..., None, None]

def inner_product(left_vec, right_vec):
    return 0.5 * lax.optimization_barrier(jnp.sum(left_vec * right_vec, axis=(0, 1, 2, 3, 4)))

def precondition(vector, precond, face_blocks, live_mask):
    partial_value = jnp.einsum('xyzbij,xyzbjr->xyzbir', precond, vector, precision=lax.Precision.HIGHEST)
    return assemble(partial_value, face_blocks, live_mask)

def operate(vector, schur, interface_diag, face_blocks, live_mask):
    subdomains = SUB_X * SUB_Y * SUB_Z
    flat_schur = schur.reshape(subdomains, IFACE, IFACE)
    flat_vector = vector.reshape(subdomains, IFACE, NRHS)
    product = lax.map(lambda pair: jnp.dot(pair[0], pair[1].astype(jnp.bfloat16), preferred_element_type=jnp.float32), (flat_schur, flat_vector))
    partial_value = product + interface_diag.reshape(subdomains, IFACE, 1) * flat_vector
    return assemble(partial_value.reshape(vector.shape), face_blocks, live_mask)

def reference(schur, interface_diag, precond, load, face_blocks):
    live_mask = find_live(face_blocks)
    block_shape = (SUB_X, SUB_Y, SUB_Z, NBLK, BLK, NRHS)
    assembled_load = assemble(load.astype(jnp.float32).reshape(block_shape), face_blocks, live_mask)
    initial = jnp.sqrt(inner_product(assembled_load, assembled_load) + epsilon)
    basis_first = assembled_load / initial
    precond_first = precondition(basis_first, precond, face_blocks, live_mask)
    working = operate(precond_first, schur, interface_diag, face_blocks, live_mask)
    diag_first = inner_product(working, basis_first)
    working = working - diag_first * basis_first
    below_first = jnp.sqrt(inner_product(working, working) + epsilon)
    basis_second = working / below_first
    precond_second = precondition(basis_second, precond, face_blocks, live_mask)
    working = operate(precond_second, schur, interface_diag, face_blocks, live_mask)
    upper_second = inner_product(working, basis_first)
    working = working - upper_second * basis_first
    diag_second = inner_product(working, basis_second)
    working = working - diag_second * basis_second
    below_second = jnp.sqrt(inner_product(working, working) + epsilon)
    radius_first = jnp.sqrt(diag_first * diag_first + below_first * below_first)
    cosine_first = diag_first / radius_first
    sine_first = below_first / radius_first
    rotated_top = cosine_first * upper_second + sine_first * diag_second
    rotated_low = cosine_first * diag_second - sine_first * upper_second
    radius_second = jnp.sqrt(rotated_low * rotated_low + below_second * below_second)
    cosine_second = rotated_low / radius_second
    sine_second = below_second / radius_second
    weight_second = -initial * sine_first * cosine_second / radius_second
    weight_first = (initial * cosine_first - rotated_top * weight_second) / radius_first
    solution = weight_first * precond_first + weight_second * precond_second
    residual_norm = initial * sine_first * sine_second
    return (solution.reshape(SUB_X, SUB_Y, SUB_Z, IFACE, NRHS), residual_norm)
```

```python
import jax
import jax.numpy as jnp
from jax import lax
from jax.experimental import pallas as pl
from jax.experimental.pallas import tpu as pltpu
from jax.sharding import PartitionSpec as P

EPS = 1e-06
B = 128
NB = 16
NS = 12
W = 128
H = 2
N = NB * B
C = NS * B
AXES = ("gx", "gy", "gz")
MESH = pl.DeviceIdType.MESH

L0, PM, L1, U10, U11, U20, U21 = range(7)


def fold(x):
    n = x.shape[0]
    while n > 8:
        n //= 2
        x = x[:n] + x[n:]
    return x


def colsum(x):
    return jnp.sum(x, axis=0, keepdims=True)


def split(x):
    hi = x.astype(jnp.bfloat16)
    lo = (x - hi.astype(jnp.float32)).astype(jnp.bfloat16)
    return hi, lo


def main_kernel(sizes, face, s_hbm, d_hbm, p_hbm, l_hbm, out, norm,
                z1, z2, sv, lb, pv, dv, sc, dcol, send_l, recv_l, r, send_p, recv_p, mhl, zb,
                u1, ru1, w1, u2, ru2, red_a, red_b, local_sem, send_sem, recv_sem,
                red_send, red_recv):
    pos = [lax.axis_index(a) for a in AXES]

    def peer(axis, index):
        ids = list(pos)
        ids[axis] = index
        return tuple(ids)

    barrier = pltpu.get_barrier_semaphore()
    peers = 0
    for axis in range(3):
        for off in range(1, sizes[axis]):
            other = lax.rem(pos[axis] + off, sizes[axis])
            pl.semaphore_signal(barrier, inc=1, device_id=peer(axis, other), device_id_type=MESH)
            peers += 1

    loads = [
        pltpu.make_async_copy(l_hbm, lb, local_sem.at[0]),
        pltpu.make_async_copy(p_hbm, pv, local_sem.at[1]),
        pltpu.make_async_copy(d_hbm, dv, local_sem.at[2]),
    ]
    loads += [
        pltpu.make_async_copy(s_hbm.at[:, :, pl.ds(t * B, B)], sv.at[t], local_sem.at[3 + t])
        for t in range(NB)
    ]
    for copy in loads:
        copy.start()

    def exists(d):
        axis = d // 2
        if d % 2 == 0:
            return pos[axis] < sizes[axis] - 1
        return pos[axis] > 0

    def slot(s):
        number = face[0, 0, 0, s // 2, s % 2]
        valid = number < NB
        return jnp.minimum(number, NB - 1), valid

    def message(m, d):
        axis = d // 2
        opp = d + 1 if d % 2 == 0 else d - 1
        step = 1 if d % 2 == 0 else sizes[axis] - 1
        other = lax.rem(pos[axis] + step, sizes[axis])
        if m in (L0, L1):
            h = 0 if m == L0 else 1
            src, dst = send_l.at[h, pl.ds(2 * d, 2)], recv_l.at[h, pl.ds(2 * opp, 2)]
        elif m == PM:
            src, dst = send_p.at[pl.ds(2 * d, 2)], recv_p.at[pl.ds(2 * opp, 2)]
        elif m in (U10, U11):
            h = m - U10
            src, dst = u1.at[h, pl.ds(2 * d, 2)], ru1.at[h, pl.ds(2 * opp, 2)]
        else:
            h = m - U20
            src, dst = u2.at[h, 2 * d + d % 2], ru2.at[h, opp]
        return pltpu.make_async_remote_copy(
            src_ref=src, dst_ref=dst, send_sem=send_sem.at[m, d], recv_sem=recv_sem.at[m, opp],
            device_id=peer(axis, other), device_id_type=MESH)

    def arrival(m, d):
        axis = d // 2
        step = 1 if d % 2 == 0 else sizes[axis] - 1
        other = lax.rem(pos[axis] + step, sizes[axis])
        if m in (L0, L1):
            h = 0 if m == L0 else 1
            src, dst = send_l.at[h, pl.ds(2 * d, 2)], recv_l.at[h, pl.ds(2 * d, 2)]
        elif m == PM:
            src, dst = send_p.at[pl.ds(2 * d, 2)], recv_p.at[pl.ds(2 * d, 2)]
        elif m in (U10, U11):
            h = m - U10
            src, dst = u1.at[h, pl.ds(2 * d, 2)], ru1.at[h, pl.ds(2 * d, 2)]
        else:
            h = m - U20
            src, dst = u2.at[h, 2 * d + d % 2], ru2.at[h, d]
        return pltpu.make_async_remote_copy(
            src_ref=src, dst_ref=dst, send_sem=send_sem.at[m, d], recv_sem=recv_sem.at[m, d],
            device_id=peer(axis, other), device_id_type=MESH)

    def send(m, d):
        @pl.when(exists(d))
        def _():
            message(m, d).start()

    def receive(m, d):
        @pl.when(exists(d))
        def _():
            arrival(m, d).wait_recv()

    loads[0].wait()
    for s in range(NS):
        block, valid = slot(s)
        mask = jnp.where(valid, 1.0, 0.0)
        rows = lb[block].astype(jnp.float32) * mask
        for h in range(H):
            send_l[h, s] = rows[:, h * W:(h + 1) * W]
    loads[1].wait()
    for s in range(NS):
        block, valid = slot(s)
        send_p[s] = pv[block] * jnp.where(valid, 1.0, 0.0)

    pl.semaphore_wait(barrier, peers)
    for m in (L0, PM, L1):
        for d in range(6):
            send(m, d)

    for d in range(6):
        @pl.when(jnp.logical_not(exists(d)))
        def _():
            zero = jnp.zeros((2, B, W), jnp.float32)
            for h in range(H):
                recv_l[h, pl.ds(2 * d, 2)] = zero
                ru1[h, pl.ds(2 * d, 2)] = zero
                ru2[h, d] = zero[0]
            recv_p[pl.ds(2 * d, 2)] = zero

    loads[2].wait()
    for s in range(NS):
        block, valid = slot(s)
        row = dv[block] * jnp.where(valid, 1.0, 0.0)
        dcol[s] = jnp.transpose(jnp.broadcast_to(row, (B, B)))

    for copy in loads[3:]:
        copy.wait()

    @pl.loop(0, 6)
    def _(d):
        for k in range(2):
            number = face[0, 0, 0, d, k]
            mask = jnp.where(number < NB, 1.0, 0.0).astype(jnp.bfloat16)
            top = jnp.minimum(number, NB - 1)
            for t in range(NS):
                block, _ = slot(t)
                sc[pl.ds(pl.multiple_of((2 * d + k) * B, B), B), t * B:(t + 1) * B] = (
                    sv[block, top] * mask)

    def apply_m(s, x):
        hi, lo = split(x)
        both = jnp.concatenate([hi, lo], axis=1)
        rhs = jnp.concatenate([both, both], axis=0)
        out = jnp.dot(mhl[s], rhs, preferred_element_type=jnp.float32)
        return out[:, :W] + out[:, W:]

    def product(h, d, z, u):
        rows = jnp.dot(sc[2 * d * B:2 * (d + 1) * B, :], zb[h], preferred_element_type=jnp.float32)
        for k in range(2):
            s = 2 * d + k
            u[h, s] = rows[k * B:(k + 1) * B] + dcol[s] * z[h, s]

    def red_copy(buf, which, axis, off, target):
        n = sizes[axis]
        return pltpu.make_async_remote_copy(
            src_ref=buf.at[axis, pos[axis]], dst_ref=buf.at[axis, target],
            send_sem=red_send.at[which, axis, off], recv_sem=red_recv.at[which, axis, off],
            device_id=peer(axis, lax.rem(pos[axis] + off, n)), device_id_type=MESH)

    def red_start(buf, which, axis, tile):
        buf[axis, pos[axis]] = tile
        for off in range(1, sizes[axis]):
            red_copy(buf, which, axis, off, pos[axis]).start()

    def red_finish(buf, which, axis):
        n = sizes[axis]
        for off in range(1, n):
            red_copy(buf, which, axis, off, lax.rem(pos[axis] - off + n, n)).wait_recv()
        total = buf[axis, 0]
        for i in range(1, n):
            total = total + buf[axis, i]
        return total

    rows_a = []
    for h in range(H):
        for d in range(6):
            receive(L0 if h == 0 else L1, d)
            if h == 0:
                receive(PM, d)
            for k in range(2):
                s = 2 * d + k
                if h == 0:
                    hi, lo = split(send_p[s] + recv_p[s])
                    mhl[s, :, :B] = hi
                    mhl[s, :, B:] = lo
                x = send_l[h, s] + recv_l[h, s]
                r[h, s] = x
                z = apply_m(s, x)
                z1[h, s] = z
                zb[h, s * B:(s + 1) * B, :] = z.astype(jnp.bfloat16)
        for d in range(6):
            product(h, d, z1, u1)
            send(U10 + h, d)
        g00 = jnp.zeros((8, W), jnp.float32)
        g01 = jnp.zeros((8, W), jnp.float32)
        for s in range(NS):
            g00 = g00 + fold(r[h, s] * r[h, s])
            g01 = g01 + fold(u1[h, s] * r[h, s])
        rows_a += [0.5 * colsum(g00), colsum(g01)]
    red_start(red_a, 0, 0, jnp.concatenate(rows_a + [jnp.zeros((4, W), jnp.float32)], axis=0))

    for h in range(H):
        for d in range(6):
            receive(U10 + h, d)
            for k in range(2):
                s = 2 * d + k
                x = u1[h, s] + ru1[h, s]
                w1[h, s] = x
                z = apply_m(s, x)
                z2[h, s] = z
                zb[h, s * B:(s + 1) * B, :] = z.astype(jnp.bfloat16)
        for d in range(6):
            product(h, d, z2, u2)
            send(U20 + h, d)
        red_start(red_a, 0, 1 + h, red_finish(red_a, 0, h))
    tot_a = red_finish(red_a, 0, 2)

    rows_b = []
    h11s = []
    for h in range(H):
        h11 = tot_a[2 * h + 1:2 * h + 2] / (tot_a[2 * h:2 * h + 1] + EPS)
        h11s.append(h11)
        gqq = jnp.zeros((8, W), jnp.float32)
        gwr = jnp.zeros((8, W), jnp.float32)
        gwq = jnp.zeros((8, W), jnp.float32)
        for s in range(NS):
            q = w1[h, s] - h11 * r[h, s]
            wq = u2[h, s] - h11 * u1[h, s]
            gqq = gqq + fold(q * q)
            gwr = gwr + fold(wq * r[h, s])
            gwq = gwq + fold(wq * q)
        rows_b.append([0.5 * colsum(gqq), colsum(gwr), colsum(gwq)])
    for h in range(H):
        gww = jnp.zeros((8, W), jnp.float32)
        for d in range(6):
            receive(U20 + h, d)
            s = 2 * d + 1 - d % 2
            v = u2[h, s] + ru2[h, d] - h11s[h] * w1[h, s]
            gww = gww + fold(v * v)
        rows_b[h].append(colsum(gww))
    tile = jnp.concatenate(rows_b[0] + rows_b[1], axis=0)
    for axis in range(3):
        red_start(red_b, 1, axis, tile)
        tile = red_finish(red_b, 1, axis)
    tot_b = tile

    c1s, c2s = [], []
    for h in range(H):
        g00, g01 = [tot_a[2 * h + i:2 * h + i + 1] for i in range(2)]
        gqq, gwr, gwq, gww = [tot_b[4 * h + i:4 * h + i + 1] for i in range(4)]
        beta2 = g00 + EPS
        beta = jnp.sqrt(beta2)
        n1 = g00 / beta2
        h11 = g01 / beta2
        q2 = gqq / beta2
        h21sq = q2 + EPS
        h21 = jnp.sqrt(h21sq)
        n2 = q2 / h21sq
        a = 1.0 / (beta * h21)
        h12 = gwr * a / beta
        h22 = gwq * a * a - h12 * (h11 * (1.0 - n1) / h21)
        ww = gww * a * a
        h32 = jnp.sqrt(jnp.maximum(
            ww - h12 * h12 * (2.0 - n1) - h22 * h22 * (2.0 - n2), 0.0) + EPS)
        r1 = jnp.sqrt(h11 * h11 + h21 * h21)
        cs1 = h11 / r1
        sn1 = h21 / r1
        top = cs1 * h12 + sn1 * h22
        low = cs1 * h22 - sn1 * h12
        r2 = jnp.sqrt(low * low + h32 * h32)
        cs2 = low / r2
        sn2 = h32 / r2
        y2 = -beta * sn1 * cs2 / r2
        y1 = (beta * cs1 - top * y2) / r1
        norm[:, h * W:(h + 1) * W] = beta * sn1 * sn2
        c2 = y2 * a
        c1s.append(y1 / beta - c2 * h11)
        c2s.append(c2)
    for b in range(NB):
        index = jnp.int32(0)
        mask = jnp.float32(0.0)
        for s in range(NS):
            hit = face[0, 0, 0, s // 2, s % 2] == b
            index = jnp.where(hit, s, index)
            mask = jnp.where(hit, 1.0, mask)
        for h in range(H):
            out[b * B:(b + 1) * B, h * W:(h + 1) * W] = mask * (
                c1s[h] * z1[h, index] + c2s[h] * z2[h, index])

    for m in range(7):
        for d in range(6):
            @pl.when(exists(d))
            def _():
                message(m, d).wait_send()
    for which, buf in ((0, red_a), (1, red_b)):
        for axis in range(3):
            for off in range(1, sizes[axis]):
                red_copy(buf, which, axis, off, pos[axis]).wait_send()


def solution(mesh):
    sizes = tuple(mesh.shape[a] for a in AXES)
    f32, bf16 = jnp.float32, jnp.bfloat16
    vmem = pl.BlockSpec(memory_space=pltpu.VMEM)
    smem = pl.BlockSpec(memory_space=pltpu.SMEM)
    hbm = pl.BlockSpec(memory_space=pltpu.HBM)
    blocks = (H, NS, B, W)

    def on_device(schur, interface_diag, precond, load, face_blocks):
        out, norm = pl.pallas_call(
            lambda *refs: main_kernel(sizes, *refs),
            out_shape=(jax.ShapeDtypeStruct((N, H * W), f32), jax.ShapeDtypeStruct((1, H * W), f32)),
            in_specs=[smem, hbm, hbm, hbm, hbm],
            out_specs=(vmem, vmem),
            scratch_shapes=[
                pltpu.VMEM(blocks, f32),
                pltpu.VMEM(blocks, f32),
                pltpu.VMEM((NB, NB, B, B), bf16),
                pltpu.VMEM((NB, B, H * W), bf16),
                pltpu.VMEM((NB, B, B), f32),
                pltpu.VMEM((NB, 1, B), f32),
                pltpu.VMEM((C, C), bf16),
                pltpu.VMEM((NS, B, W), f32),
                pltpu.VMEM(blocks, f32),
                pltpu.VMEM(blocks, f32),
                pltpu.VMEM(blocks, f32),
                pltpu.VMEM((NS, B, B), f32),
                pltpu.VMEM((NS, B, B), f32),
                pltpu.VMEM((NS, B, 2 * B), bf16),
                pltpu.VMEM((H, C, W), bf16),
                pltpu.VMEM(blocks, f32),
                pltpu.VMEM(blocks, f32),
                pltpu.VMEM(blocks, f32),
                pltpu.VMEM(blocks, f32),
                pltpu.VMEM((H, 6, B, W), f32),
                pltpu.VMEM((3, 8, 8, W), f32),
                pltpu.VMEM((3, 8, 8, W), f32),
                pltpu.SemaphoreType.DMA((3 + NB,)),
                pltpu.SemaphoreType.DMA((7, 6)),
                pltpu.SemaphoreType.DMA((7, 6)),
                pltpu.SemaphoreType.DMA((2, 3, 8)),
                pltpu.SemaphoreType.DMA((2, 3, 8)),
            ],
            compiler_params=pltpu.CompilerParams(
                collective_id=0, has_side_effects=True, vmem_limit_bytes=46 * 1024 * 1024),
            name="gmres_steps",
        )(face_blocks, schur.reshape(NB, B, N), interface_diag.reshape(NB, 1, B),
          precond.reshape(NB, B, B), load.reshape(NB, B, H * W))
        return out.reshape(1, 1, 1, N, H * W), norm.reshape(H * W)

    in_specs = (
        P("gx", "gy", "gz", None, None),
        P("gx", "gy", "gz", None),
        P("gx", "gy", "gz", None, None, None),
        P("gx", "gy", "gz", None, None),
        P("gx", "gy", "gz", None, None),
    )
    out_specs = (P("gx", "gy", "gz", None, None), P(None))
    return jax.shard_map(on_device, mesh=mesh, in_specs=in_specs, out_specs=out_specs,
                         check_vma=False)
```
